32 devices in a mesh: dp: 8 (over y, x, core), seq: 4 (over z).
Axes of the slice: x: 2, y: 2, z: 4, core: 2. Of those that a mesh axis runs over, the one named last changes fastest.
Arguments:
- qkv: bfloat16 [16, 1024, 4608], P('dp', 'seq'), may hold values from -20.4 to 20.4
- gate: float32 [16, 3072], P('dp'), may hold values from 0.5 to 2.5
- cotangent: bfloat16 [16, 1024, 3072], P('dp', 'seq'), may hold values from -6 to 6
- out_weight: bfloat16 [1536, 3072], replicated, may hold values from -0.15625 to 0.15625
- clip_lengths: int32 [16], replicated, may hold values from 1 to 768, as said below
- text_lengths: int32 [16], replicated, may hold values from 1 to 256, as said below
- plan: int32 [8], replicated, may hold values from 0 to 7, as said below
Outputs:
- mixed: bfloat16 [16, 1024, 3072], P('dp', 'seq')
- gate_grad: float32 [16, 3072], P('dp')
- weight_grad: float32 [1536, 3072], P(None, ('dp', 'seq'))
- qkv_grad: bfloat16 [16, 1024, 4608], P('dp', 'seq')
The draws below stay inside these ranges and needn't reach their ends.
Inputs may be any that keep to these rules, and one draw needn't show every extreme that they name: clip_lengths[c] counts the live video positions of source clip c = 2 g + s (group g, slot s); some clip has exactly 768. text_lengths[c] counts the live text positions of source clip c; some clip has exactly 256. plan is a permutation of 0 to 7: the second clip of group g becomes the second clip of group plan[g].
All inputs are finite; a program needn't handle non-finite values.
Results may differ from the reference program's by a relative error of at most 0.011.
Values may be sent and summed in bfloat16 or wider, within the bound.
A program may use at most 128 MiB of HBM per device.

```python
import jax
import jax.numpy as jnp
from jax import lax

D = 3072
HEADS = 12
HD = 128
TXT = 256
CLIP = 768
GROUPS = 8
CLIPS = 16
SEQ = 1024


def draw_qkv(key, part):
    head_width = HEADS * HD
    full_width = 3 * head_width
    normal_draw = jnp.clip(jax.random.normal(key, (CLIPS, SEQ, full_width), jnp.float32), -6.0, 6.0)
    return normal_draw.astype(jnp.bfloat16)


def length_table(key):
    folded = jax.random.fold_in(key, 11)
    k_heavy, k_long, k_short, k_peak = jax.random.split(folded, 4)
    heavier = jax.random.randint(k_heavy, (GROUPS, 1), 0, 2)
    longer = jax.random.randint(k_long, (GROUPS, 2), CLIP // 2 + 1, CLIP + 1)
    shorter = jax.random.randint(k_short, (GROUPS, 2), 1, CLIP // 4 + 1)
    lengths_all = jnp.where(heavier == 1, longer, shorter).reshape(CLIPS)
    peak_index = jax.random.randint(k_peak, (), 0, CLIPS)
    return jnp.where(jnp.arange(CLIPS) == peak_index, CLIP, lengths_all).astype(jnp.int32)


def draw_clip_lengths(key, part):
    return length_table(key)


def draw_plan(key, part):
    lengths_all = length_table(key)
    ordinal = jnp.arange(GROUPS, dtype=jnp.int32)
    first_keys = lengths_all[0::2] * GROUPS + ordinal
    second = lengths_all[1::2] * GROUPS + ordinal
    longest = jnp.argsort(-first_keys, stable=True).astype(jnp.int32)
    shortest = jnp.argsort(second, stable=True).astype(jnp.int32)
    return jnp.zeros((GROUPS,), jnp.int32).at[shortest].set(longest)


def draw_text_lengths(key, part):
    folded = jax.random.fold_in(key, 23)
    k_draw, k_peak = jax.random.split(folded, 2)
    lengths_all = jax.random.randint(k_draw, (CLIPS,), 1, TXT + 1)
    peak_index = jax.random.randint(k_peak, (), 0, CLIPS)
    return jnp.where(jnp.arange(CLIPS) == peak_index, TXT, lengths_all).astype(jnp.int32)


def level_of(key, shape, shards, low, top_value):
    def one(position, blocks):
        heights = jax.random.uniform(jax.random.fold_in(jax.random.fold_in(key, 6), position), (blocks,), jnp.float32, low / len(shards), top_value / len(shards))
        return jnp.repeat(jnp.exp(heights), shape[position] // blocks).reshape((-1,) + (1,) * (len(shape) - position - 1))

    gain = one(*shards[0])
    for cut in shards[1:]:
        gain = gain * one(*cut)
    return gain


def bell_draw(stream_key, dims, spread, limit, cuts=(), kind=jnp.bfloat16):
    drawn = jax.random.normal(stream_key, dims, jnp.float32) * spread
    if len(cuts) > 0:
        drawn = level_of(stream_key, dims, cuts, -0.22, 0.18) * drawn
    return jnp.clip(drawn, min=-limit, max=limit).astype(kind)


def setup_inputs(seed: int = 0) -> dict:
    streams_of = jax.random.split(jax.random.key(seed), 8)
    qkv = draw_qkv(jax.random.fold_in(streams_of[7], 71), 0)
    gate = jnp.clip(0.5 + 2.0 * jax.random.uniform(streams_of[1], (CLIPS, D), jnp.float32) ** level_of(streams_of[1], (CLIPS, D), ((0, 8),), -0.2, 0.2), 0.5, 2.5)
    cotangent = bell_draw(streams_of[2], (CLIPS, SEQ, D), 1.0, 6.0, ((0, 8), (1, 4)))
    out_weight = bell_draw(streams_of[3], (HEADS * HD, D), (HEADS * HD) ** -0.5, 0.15625)
    clip_lengths = draw_clip_lengths(jax.random.fold_in(streams_of[7], 71), 0)
    text_lengths = draw_text_lengths(jax.random.fold_in(streams_of[7], 71), 0)
    plan = draw_plan(jax.random.fold_in(streams_of[7], 71), 0)
    return {"qkv": qkv, "gate": gate, "cotangent": cotangent, "out_weight": out_weight, "clip_lengths": clip_lengths, "text_lengths": text_lengths, "plan": plan}


NEGATIVE = -1e30


def allowed_rows(text_len, video_len):
    places = jnp.arange(SEQ, dtype=jnp.int32)
    return (places < text_len) | ((places >= TXT) & (places < TXT + video_len))


def reference(qkv, gate, cotangent, out_weight, clip_lengths, text_lengths, plan):
    head_width = HEADS * HD
    ordinal = jnp.arange(GROUPS, dtype=jnp.int32)
    inverse = jnp.zeros((GROUPS,), jnp.int32).at[plan].set(ordinal)
    source_of = jnp.stack([2 * ordinal, 2 * inverse + 1], axis=1).reshape(CLIPS).astype(jnp.int32)
    score_scale = HD ** -0.5

    def clip_step(weight_sum, inputs):
        tokens, gate_row, grad_row, text_len, video_len = inputs
        allowed = allowed_rows(text_len, video_len)
        live_pairs = (allowed[:, None] & allowed[None, :])[None]
        queries = tokens[:, :head_width].reshape(SEQ, HEADS, HD).astype(jnp.float32)
        keys_all = tokens[:, head_width:2 * head_width].reshape(SEQ, HEADS, HD).astype(jnp.float32)
        values_all = tokens[:, 2 * head_width:].reshape(SEQ, HEADS, HD).astype(jnp.float32)
        scores = jnp.einsum('qhd,khd->hqk', queries, keys_all) * score_scale
        masked = jnp.where(live_pairs, scores, NEGATIVE)
        row_peak = jnp.max(masked, axis=-1, keepdims=True)
        row_total = jnp.sum(jnp.exp(masked - row_peak), axis=-1, keepdims=True)
        log_total = row_peak + jnp.log(row_total)
        probabilities = jnp.exp(jnp.where(live_pairs, scores - log_total, NEGATIVE))
        probs_low = lax.optimization_barrier(probabilities.astype(jnp.bfloat16))
        attended = jnp.einsum('hqk,khd->qhd', probs_low.astype(jnp.float32), values_all).astype(jnp.bfloat16)
        attended = lax.optimization_barrier(attended)
        attended_flat = attended.reshape(SEQ, head_width)
        outputs = jnp.dot(attended_flat, out_weight, preferred_element_type=jnp.float32)
        mixed = (gate_row[None, :] * outputs).astype(jnp.bfloat16)
        gate_grad = jnp.sum(grad_row.astype(jnp.float32) * outputs, axis=0)
        scaled = (grad_row.astype(jnp.float32) * gate_row[None, :]).astype(jnp.bfloat16)
        weight_sum = weight_sum + jnp.dot(attended_flat.T, scaled, preferred_element_type=jnp.float32)
        d_attn = jnp.dot(scaled, out_weight.T, preferred_element_type=jnp.float32).astype(jnp.bfloat16)
        d_attn = lax.optimization_barrier(d_attn)
        d_heads = d_attn.reshape(SEQ, HEADS, HD).astype(jnp.float32)
        row_dots = jnp.einsum('qhd,qhd->hq', d_heads, attended.astype(jnp.float32))
        d_probs = jnp.einsum('qhd,khd->hqk', d_heads, values_all)
        d_scores = lax.optimization_barrier((probabilities * (d_probs - row_dots[..., None])).astype(jnp.bfloat16))
        d_scores = d_scores.astype(jnp.float32)
        grad_q = jnp.einsum('hqk,khd->qhd', d_scores, keys_all) * score_scale
        grad_k = jnp.einsum('hqk,qhd->khd', d_scores, queries) * score_scale
        grad_v = jnp.einsum('hqk,qhd->khd', probs_low.astype(jnp.float32), d_heads)
        gradients = jnp.concatenate([grad_q.reshape(SEQ, head_width), grad_k.reshape(SEQ, head_width), grad_v.reshape(SEQ, head_width)], axis=1).astype(jnp.bfloat16)
        return weight_sum, (mixed, gate_grad, gradients)

    scan_inputs = (qkv[source_of], gate, cotangent, text_lengths[source_of], clip_lengths[source_of])
    weight_grad, (mixed, gate_grad, balanced_grads) = lax.scan(clip_step, jnp.zeros((head_width, D), jnp.float32), scan_inputs)
    qkv_grad = jnp.zeros_like(qkv).at[source_of].set(balanced_grads)
    return mixed, gate_grad, weight_grad, qkv_grad
```

```python
import functools
import math

import jax
import jax.numpy as jnp
from jax import lax
from jax.experimental import pallas as pl
from jax.experimental.pallas import tpu as pltpu
from jax.sharding import PartitionSpec as P

HD = 128
TXT = 256
BLOCK = 256
WIDE = 512
NEGATIVE = -1e30
LOG2E = math.log2(math.e)
MESH = pl.DeviceIdType.MESH


def dot(left, right, left_dim, right_dim):
    return lax.dot_general(
        left, right, (((left_dim,), (right_dim,)), ((), ())), preferred_element_type=jnp.float32
    )


def live_places(places, text_len, video_len):
    return (places < text_len) | ((places >= TXT) & (places < TXT + video_len))


def aligned(start, size, unit=128):
    return pl.ds(pl.multiple_of(start, unit), size)


def bit_of(index, bit):
    return (index // (1 << bit)) % 2


def rest_value(count, taken, bits):
    value = 0
    for bit in range(bits):
        if bit not in taken:
            value += (count % 2) << bit
            count //= 2
    return value


def block_kernel(
    groups, ways,
    clip_ref, text_ref, plan_ref, gate_ref, qkv_ref, cot_ref, w_hbm,
    mixed_ref, gate_out, weight_out, grad_ref,
    w, cot, scaled, tok, heads_d, flat_d, land_o, even_o,
    parts_d, spread_d, pick_d, home_d, parts_o, spread_o, pick_o, home_o,
    partial, near, mid, low, z_near, z_far, gate_all, bias, dk_sum, dv_sum,
    load_sem, own_sem, out_sem,
    in_send, in_recv, d_send, d_recv, o_send, o_recv, g_send, g_recv,
    dp_send, dp_recv, rs_send, rs_recv, zw_send, zw_recv, gate_send, gate_recv,
):
    group, place = lax.axis_index("dp"), lax.axis_index("seq")
    rows, model = cot.shape[1], cot.shape[2]
    width = flat_d.shape[2]
    local = width // ways
    heads = local // HD
    seq_len = rows * ways
    part = rows // groups
    dp_bits = groups.bit_length() - 1
    z_order = sorted(range(1, ways), key=lambda k: -min(k, ways - k))
    my_rows = aligned(place * rows, rows, rows)

    barrier = pltpu.get_barrier_semaphore()
    for k in range(1, ways):
        pl.semaphore_signal(
            barrier, inc=1, device_id={"seq": lax.rem(place + k, ways)}, device_id_type=MESH
        )
    for k in range(1, groups):
        pl.semaphore_signal(
            barrier, inc=1, device_id={"dp": lax.rem(group + k, groups)}, device_id_type=MESH
        )
    pl.semaphore_wait(barrier, ways + groups - 2)

    sent = []

    def start(copy):
        copy.start()
        sent.append(copy)

    def to_z(source, target, send, recv, k):
        return pltpu.make_async_remote_copy(
            source, target, send, recv, {"seq": lax.rem(place + k, ways)}, MESH
        )

    def qkv_copy(slot, member, k):
        peer = lax.rem(place + k, ways)
        return to_z(
            qkv_ref.at[slot, :, aligned(member * width + peer * local, local)],
            tok.at[slot, my_rows, pl.ds(member * local, local)],
            in_send.at[slot, member, k - 1], in_recv.at[slot, member, k - 1], k,
        )

    def qkv_own(slot, member):
        return pltpu.make_async_copy(
            qkv_ref.at[slot, :, aligned(member * width + place * local, local)],
            tok.at[slot, my_rows, pl.ds(member * local, local)],
            own_sem.at[slot, member],
        )

    def d_copy(slot, k):
        peer = lax.rem(place + k, ways)
        return to_z(
            flat_d.at[slot, :, aligned(peer * local, local)], heads_d.at[slot, my_rows, :],
            d_send.at[slot, k - 1], d_recv.at[slot, k - 1], k,
        )

    def d_own(slot):
        return pltpu.make_async_copy(
            flat_d.at[slot, :, aligned(place * local, local)], heads_d.at[slot, my_rows, :],
            own_sem.at[slot, 3],
        )

    def o_copy(slot, head, k):
        peer = lax.rem(place + k, ways)
        return to_z(
            heads_d.at[slot, aligned(peer * rows, rows, rows), aligned(head * HD, HD)],
            land_o.at[slot, :, aligned(place * local + head * HD, HD)],
            o_send.at[slot, head, k - 1], o_recv.at[slot, head, k - 1], k,
        )

    def o_own(slot):
        return pltpu.make_async_copy(
            heads_d.at[slot, my_rows, :], land_o.at[slot, :, aligned(place * local, local)],
            own_sem.at[slot, 4],
        )

    def grad_copy(slot, member, k):
        peer = lax.rem(place + k, ways)
        return to_z(
            tok.at[slot, aligned(peer * rows, rows, rows), pl.ds(member * local, local)],
            grad_ref.at[slot, :, aligned(member * width + place * local, local)],
            g_send.at[slot, member, k - 1], g_recv.at[slot, member, k - 1], k,
        )

    def grad_own(slot, member):
        return pltpu.make_async_copy(
            tok.at[slot, my_rows, pl.ds(member * local, local)],
            grad_ref.at[slot, :, aligned(member * width + place * local, local)],
            own_sem.at[slot, 5 + member],
        )

    def dp_copy(source, target, which, k):
        peer = lax.rem(group + k, groups)
        return pltpu.make_async_remote_copy(
            source.at[peer], target.at[group],
            dp_send.at[which, k - 1], dp_recv.at[which, k - 1], {"dp": peer}, MESH,
        )

    def spread_start(source, target, which):
        for k in range(1, groups):
            start(dp_copy(source, target, which, k))
        target[group] = source[group]

    def spread_wait(source, target, which):
        for k in range(1, groups):
            dp_copy(source, target, which, k).wait_recv()

    def split_rows(source, slot, target):
        for index in range(groups):
            piece = source[slot].astype(jnp.float32)[index * part:(index + 1) * part]
            target[index] = piece.astype(jnp.bfloat16)

    def merge_rows(source, target, slot):
        merged = source[...].astype(jnp.float32).reshape(rows, width)
        target[slot] = merged.astype(jnp.bfloat16)

    def scale_rows(slot):
        def step(index, carry):
            columns = aligned(index * WIDE, WIDE)
            values = cot[slot, :, columns].astype(jnp.float32) * gate_ref[slot:slot + 1, columns]
            scaled[slot, :, columns] = values.astype(jnp.bfloat16)
            return carry

        lax.fori_loop(0, model // WIDE, step, 0)

    def back_project(slot):
        def step(index, carry):
            columns = aligned(index * BLOCK, BLOCK, BLOCK)
            flat_d[slot, :, columns] = dot(scaled[slot], w[columns, :], 1, 1).astype(jnp.bfloat16)
            return carry

        lax.fori_loop(0, width // BLOCK, step, 0)

    def attend(slot):
        text_len, video_len = text_ref[2 * group + slot], clip_ref[2 * group + slot]
        scale = HD ** (-0.5)
        places = lax.broadcasted_iota(jnp.int32, bias.shape, 0)
        bias[...] = jnp.where(live_places(places, text_len, video_len), 0.0, NEGATIVE)

        def head_step(head, carry):
            columns = aligned(head * HD, HD)
            k_columns = aligned(local + head * HD, HD)
            v_columns = aligned(2 * local + head * HD, HD)

            def step(block, inner):
                span = aligned(block * BLOCK, BLOCK, BLOCK)
                q_rows, d_rows = tok[slot, span, columns], heads_d[slot, span, columns]
                keys, values = tok[slot, :, k_columns], tok[slot, :, v_columns]
                scores = dot(keys, q_rows, 1, 1) * (scale * LOG2E) + bias[...]
                peak = jnp.max(scores, axis=0, keepdims=True)
                weights = jnp.exp2(scores - peak)
                total = jnp.sum(weights, axis=0, keepdims=True)
                spots = block * BLOCK + lax.broadcasted_iota(jnp.int32, (1, BLOCK), 1)
                share = jnp.where(live_places(spots, text_len, video_len), 1.0 / total, 0.0)
                probs = weights * share
                probs_low = probs.astype(jnp.bfloat16)
                attended = dot(values, probs_low, 0, 0).T.astype(jnp.bfloat16)
                products = d_rows.astype(jnp.float32) * attended.astype(jnp.float32)
                row_dots = jnp.sum(products.T, axis=0, keepdims=True)
                d_probs = dot(values, d_rows, 1, 1)
                d_scores = (probs * (d_probs - row_dots)).astype(jnp.bfloat16)
                v_part = dot(probs_low, d_rows, 1, 0)
                k_part = dot(d_scores, q_rows, 1, 0)
                q_part = dot(keys, d_scores, 0, 0).T
                tok[slot, span, columns] = (q_part * scale).astype(jnp.bfloat16)
                heads_d[slot, span, columns] = attended

                @pl.when(block == 0)
                def _():
                    dk_sum[...] = k_part
                    dv_sum[...] = v_part

                @pl.when(block > 0)
                def _():
                    dk_sum[...] += k_part
                    dv_sum[...] += v_part

                return inner

            lax.fori_loop(0, seq_len // BLOCK, step, 0)
            tok[slot, :, k_columns] = (dk_sum[...] * scale).astype(jnp.bfloat16)
            tok[slot, :, v_columns] = dv_sum[...].astype(jnp.bfloat16)
            for k in z_order:
                o_copy(slot, head, k).start()
            return carry

        lax.fori_loop(0, heads, head_step, 0)
        o_own(slot).start()

    def o_wait(slot):
        o_own(slot).wait()
        for head in range(heads):
            for k in z_order:
                o_copy(slot, head, k).wait_recv()

    def qkv_start(slot):
        for member in range(3):
            for k in z_order:
                start(qkv_copy(slot, member, k))
            qkv_own(slot, member).start()

    def d_start(slot):
        for k in z_order:
            start(d_copy(slot, k))
        d_own(slot).start()

    def in_wait(slot):
        for member in range(3):
            qkv_own(slot, member).wait()
            for k in z_order:
                qkv_copy(slot, member, k).wait_recv()
        d_own(slot).wait()
        for k in z_order:
            d_copy(slot, k).wait_recv()

    def grad_start(slot, member):
        for k in z_order:
            start(grad_copy(slot, member, k))
        grad_own(slot, member).start()

    cot_load = pltpu.make_async_copy(cot_ref, cot, load_sem.at[0])
    w_load = pltpu.make_async_copy(w_hbm, w, load_sem.at[1])
    qkv_start(1)
    cot_load.start()
    w_load.start()
    cot_load.wait()
    scale_rows(1)
    w_load.wait()
    back_project(1)
    split_rows(flat_d, 1, parts_d)
    spread_start(parts_d, spread_d, 0)
    scale_rows(0)
    back_project(0)
    spread_wait(parts_d, spread_d, 0)
    for index in range(groups):
        pick_d[index] = spread_d[plan_ref[index]]
    spread_start(pick_d, home_d, 1)
    spread_wait(pick_d, home_d, 1)
    merge_rows(home_d, flat_d, 1)
    d_start(1)
    qkv_start(0)
    d_start(0)

    in_wait(1)
    attend(1)
    in_wait(0)
    attend(0)
    for member in range(3):
        grad_start(1, member)
    for member in range(2):
        grad_start(0, member)

    o_wait(1)
    split_rows(land_o, 1, parts_o)
    spread_start(parts_o, spread_o, 2)
    spread_wait(parts_o, spread_o, 2)
    for index in range(groups):
        origin = 0
        for other in range(groups):
            origin = jnp.where(plan_ref[other] == index, other, origin)
        pick_o[index] = spread_o[origin]
    spread_start(pick_o, home_o, 3)
    o_wait(0)
    spread_wait(pick_o, home_o, 3)
    merge_rows(home_o, even_o, 0)

    block_rows = model // groups
    per_step = max(1, 384 // block_rows)
    piece_rows = block_rows // ways

    def weight_step(index):
        columns = aligned(index * (per_step * block_rows), per_step * block_rows)
        value = dot(scaled[0, :, columns], land_o[0], 0, 0)
        value += dot(scaled[1, :, columns], even_o[0], 0, 0)
        for inner in range(per_step):
            for way in range(ways):
                first = (inner * ways + way) * piece_rows
                partial[index * per_step + inner, way] = (
                    value[first:first + piece_rows].astype(jnp.bfloat16)
                )

    halves = (pl.ds(0, width // 2), pl.ds(width // 2, width // 2))
    orders = (list(range(dp_bits)), [0] + list(range(dp_bits - 1, 0, -1)))
    stages = []
    count = 0
    for stage in range(dp_bits):
        entries = []
        for half in range(2):
            order = orders[half]
            taken = order[:stage + 1]
            bit = order[stage]
            kept = sum((bit_of(group, other) << other for other in order[:stage]), 0)
            for index in range(groups >> (stage + 1)):
                rest = rest_value(index, taken, dp_bits)
                given = kept + (1 - bit_of(group, bit)) * (1 << bit) + rest
                held = kept + bit_of(group, bit) * (1 << bit) + rest
                entries.append((half, bit, index, given, held, count))
                count += 1
        stages.append(entries)

    def landed(stage, index, columns):
        if stage == 0:
            return near.at[index, :, :, columns]
        if stage == 1:
            return mid.at[index, :, :, columns]
        first = sum(groups >> (other + 1) for other in range(2, stage))
        return low.at[first + index, :, :, columns]

    def rs_copy(stage, entry):
        half, bit, index, given, _, number = entry
        partner = group + (1 - 2 * bit_of(group, bit)) * (1 << bit)
        return pltpu.make_async_remote_copy(
            partial.at[given, :, :, halves[half]], landed(stage, index, halves[half]),
            rs_send.at[number], rs_recv.at[number], {"dp": partner}, MESH,
        )

    def rs_start(stage):
        for entry in stages[stage]:
            start(rs_copy(stage, entry))

    def rs_finish(stage):
        for entry in stages[stage]:
            rs_copy(stage, entry).wait_recv()
            half, _, index, _, held, _ = entry
            arrived = landed(stage, index, halves[half])

            def step(way, carry):
                value = partial[held, way, :, halves[half]].astype(jnp.float32)
                value += arrived[way].astype(jnp.float32)
                partial[held, way, :, halves[half]] = value.astype(jnp.bfloat16)
                return carry

            lax.fori_loop(0, ways, step, 0)

    steps = groups // per_step
    mine = bit_of(group, 0)
    if per_step == 1:
        def far_step(index, carry):
            weight_step(2 * index + (1 - mine))
            return carry

        def near_step(index, carry):
            weight_step(2 * index + mine)
            return carry

        lax.fori_loop(0, steps // 2, far_step, 0)
        rs_start(0)
        lax.fori_loop(0, steps // 2, near_step, 0)
    else:
        def any_step(index, carry):
            weight_step(index)
            return carry

        lax.fori_loop(0, steps, any_step, 0)
        rs_start(0)

    def project(slot, rows_ref, row_slot):
        def step(index, carry):
            columns = aligned(index * WIDE, WIDE)
            outputs = dot(rows_ref[row_slot], w[:, columns], 1, 0)
            arriving = cot[slot, :, columns].astype(jnp.float32)
            gate_all[place, slot:slot + 1, columns] = jnp.sum(
                arriving * outputs, axis=0, keepdims=True
            )
            gated = outputs * gate_ref[slot:slot + 1, columns]
            cot[slot, :, columns] = gated.astype(jnp.bfloat16)
            return carry

        lax.fori_loop(0, model // WIDE, step, 0)
        pltpu.make_async_copy(cot.at[slot], mixed_ref.at[slot], out_sem.at[slot]).start()

    def gate_copy(k):
        return to_z(
            gate_all.at[place], gate_all.at[place], gate_send.at[k - 1], gate_recv.at[k - 1], k
        )

    rs_finish(0)
    rs_start(1)
    project(0, land_o, 0)
    project(1, even_o, 0)
    rs_finish(1)
    for stage in range(2, dp_bits):
        rs_start(stage)
        rs_finish(stage)

    z_low = bit_of(place, 0)
    z_high = bit_of(place, 1)
    half_ways = ways // 2

    def near_copy(index):
        return pltpu.make_async_remote_copy(
            partial.at[group, 2 * index + (1 - z_low)], z_near.at[index],
            zw_send.at[index], zw_recv.at[index], {"seq": place + 1 - 2 * z_low}, MESH,
        )

    for index in range(half_ways):
        start(near_copy(index))
    grad_start(0, 2)
    for k in z_order:
        start(gate_copy(k))
    for index in range(half_ways):
        near_copy(index).wait_recv()
        held = 2 * index + z_low
        value = partial[group, held].astype(jnp.float32) + z_near[index].astype(jnp.float32)
        partial[group, held] = value.astype(jnp.bfloat16)
    far_copy = pltpu.make_async_remote_copy(
        partial.at[group, 2 * (1 - z_high) + z_low], z_far,
        zw_send.at[half_ways], zw_recv.at[half_ways], {"seq": place + 2 - 4 * z_high}, MESH,
    )
    start(far_copy)
    for k in z_order:
        gate_copy(k).wait_recv()
    gate_out[...] = jnp.sum(gate_all[...], axis=0)
    far_copy.wait_recv()
    weight_out[...] = partial[group, place].astype(jnp.float32) + z_far[...].astype(jnp.float32)

    for slot in (0, 1):
        pltpu.make_async_copy(cot.at[slot], mixed_ref.at[slot], out_sem.at[slot]).wait()
        for member in range(3):
            grad_own(slot, member).wait()
            for k in z_order:
                grad_copy(slot, member, k).wait_recv()
        for head in range(heads):
            for k in z_order:
                o_copy(slot, head, k).wait_send()
    for copy in sent:
        copy.wait_send()


def body(qkv, gate, cotangent, out_weight, clip_lengths, text_lengths, plan):
    groups, ways = lax.axis_size("dp"), lax.axis_size("seq")
    slots, rows, full = qkv.shape
    width, model = out_weight.shape
    local, heads = width // ways, width // ways // HD
    seq_len, part = rows * ways, rows // groups
    piece = model // groups // ways
    low = jnp.bfloat16
    dp_bits = groups.bit_length() - 1
    reduced = sum(2 * (groups >> (stage + 1)) for stage in range(dp_bits))
    late = max(1, sum(groups >> (stage + 1) for stage in range(2, dp_bits)))
    dma = pltpu.SemaphoreType.DMA
    split = pltpu.VMEM((groups, part, width), low)
    scratch = [
        pltpu.VMEM((width, model), low),
        pltpu.VMEM((slots, rows, model), low),
        pltpu.VMEM((slots, rows, model), low),
        pltpu.VMEM((slots, seq_len, 3 * local), low),
        pltpu.VMEM((slots, seq_len, local), low),
        pltpu.VMEM((slots, rows, width), low),
        pltpu.VMEM((slots, rows, width), low),
        pltpu.VMEM((1, rows, width), low),
    ] + [split] * 8 + [
        pltpu.VMEM((groups, ways, piece, width), low),
        pltpu.VMEM((groups // 2, ways, piece, width), low),
        pltpu.VMEM((groups // 4, ways, piece, width), low),
        pltpu.VMEM((late, ways, piece, width), low),
        pltpu.VMEM((ways // 2, piece, width), low),
        pltpu.VMEM((piece, width), low),
        pltpu.VMEM((ways, slots, model), jnp.float32),
        pltpu.VMEM((seq_len, BLOCK), jnp.float32),
        pltpu.VMEM((seq_len, HD), jnp.float32),
        pltpu.VMEM((seq_len, HD), jnp.float32),
        dma((2,)), dma((slots, 8)), dma((slots,)),
    ]
    for shape in (
        (slots, 3, ways - 1), (slots, ways - 1), (slots, heads, ways - 1), (slots, 3, ways - 1),
        (4, groups - 1), (reduced,), (ways // 2 + 1,), (ways - 1,),
    ):
        scratch += [dma(shape), dma(shape)]
    smem, vmem, anywhere = (
        pl.BlockSpec(memory_space=space) for space in (pltpu.SMEM, pltpu.VMEM, pl.ANY)
    )
    mixed, gate_grad, weight_rows, qkv_grad = pl.pallas_call(
        functools.partial(block_kernel, groups, ways),
        in_specs=[smem] * 3 + [vmem] + [anywhere] * 3,
        out_specs=[anywhere, vmem, vmem, anywhere],
        out_shape=[
            jax.ShapeDtypeStruct(cotangent.shape, low),
            jax.ShapeDtypeStruct(gate.shape, jnp.float32),
            jax.ShapeDtypeStruct((piece, width), jnp.float32),
            jax.ShapeDtypeStruct(qkv.shape, low),
        ],
        scratch_shapes=scratch,
        compiler_params=pltpu.CompilerParams(
            collective_id=0, has_side_effects=True, vmem_limit_bytes=67_000_000
        ),
        name="attention_half",
    )(clip_lengths, text_lengths, plan, gate, qkv, cotangent, out_weight)
    return mixed, gate_grad, weight_rows.T, qkv_grad


def solution(mesh):
    in_specs = (P("dp", "seq", None), P("dp", None), P("dp", "seq", None), P(), P(), P(), P())
    out_specs = (P("dp", "seq", None), P("dp", None), P(None, ("dp", "seq")), P("dp", "seq", None))
    return jax.shard_map(body, mesh=mesh, in_specs=in_specs, out_specs=out_specs, check_vma=False)
```

```python
import functools
import math

import jax
import jax.numpy as jnp
from jax import lax
from jax.experimental import pallas as pl
from jax.experimental.pallas import tpu as pltpu
from jax.sharding import PartitionSpec as P

HD = 128
TXT = 256
BLOCK = 256
WIDE = 512
NEGATIVE = -1e30
LOG2E = math.log2(math.e)
MESH = pl.DeviceIdType.MESH


def dot(left, right, left_dim, right_dim):
    return lax.dot_general(
        left, right, (((left_dim,), (right_dim,)), ((), ())), preferred_element_type=jnp.float32
    )


def live_places(places, text_len, video_len):
    return (places < text_len) | ((places >= TXT) & (places < TXT + video_len))


def aligned(start, size, unit=128):
    return pl.ds(pl.multiple_of(start, unit), size)


def bit_of(index, bit):
    return (index // (1 << bit)) % 2


def rest_value(count, taken, bits):
    value = 0
    for bit in range(bits):
        if bit not in taken:
            value += (count % 2) << bit
            count //= 2
    return value


def block_kernel(
    groups, ways,
    clip_ref, text_ref, plan_ref, gate_ref, qkv_ref, cot_ref, w_hbm,
    cot, gate_out, weight_out, grad_ref,
    w, scaled, tok, heads_d, flat_d, land_o,
    parts, spread, home,
    partial, near, mid, low, z_near, z_far, gate_all, bias, dk_sum, dv_sum,
    load_sem, own_sem,
    in_send, in_recv, d_send, d_recv, o_send, o_recv, g_send, g_recv,
    dp_send, dp_recv, rs_send, rs_recv, zw_send, zw_recv, gate_send, gate_recv,
):
    group, place = lax.axis_index("dp"), lax.axis_index("seq")
    rows, model = cot.shape[1], cot.shape[2]
    width = flat_d.shape[2]
    local = width // ways
    heads = local // HD
    seq_len = rows * ways
    part = rows // groups
    dp_bits = groups.bit_length() - 1
    z_order = sorted(range(1, ways), key=lambda k: -min(k, ways - k))
    my_rows = aligned(place * rows, rows, rows)

    barrier = pltpu.get_barrier_semaphore()
    for k in range(1, ways):
        pl.semaphore_signal(
            barrier, inc=1, device_id={"seq": lax.rem(place + k, ways)}, device_id_type=MESH
        )
    for k in range(1, groups):
        pl.semaphore_signal(
            barrier, inc=1, device_id={"dp": lax.rem(group + k, groups)}, device_id_type=MESH
        )
    pl.semaphore_wait(barrier, ways + groups - 2)

    sent = []

    def start(copy):
        copy.start()
        sent.append(copy)

    def to_z(source, target, send, recv, k):
        return pltpu.make_async_remote_copy(
            source, target, send, recv, {"seq": lax.rem(place + k, ways)}, MESH
        )

    def qkv_copy(slot, member, k):
        peer = lax.rem(place + k, ways)
        return to_z(
            qkv_ref.at[slot, :, aligned(member * width + peer * local, local)],
            tok.at[slot, my_rows, pl.ds(member * local, local)],
            in_send.at[slot, member, k - 1], in_recv.at[slot, member, k - 1], k,
        )

    def qkv_own(slot, member):
        return pltpu.make_async_copy(
            qkv_ref.at[slot, :, aligned(member * width + place * local, local)],
            tok.at[slot, my_rows, pl.ds(member * local, local)],
            own_sem.at[slot, member],
        )

    def d_copy(slot, k):
        peer = lax.rem(place + k, ways)
        return to_z(
            flat_d.at[slot, :, aligned(peer * local, local)], heads_d.at[slot, my_rows, :],
            d_send.at[slot, k - 1], d_recv.at[slot, k - 1], k,
        )

    def d_own(slot):
        return pltpu.make_async_copy(
            flat_d.at[slot, :, aligned(place * local, local)], heads_d.at[slot, my_rows, :],
            own_sem.at[slot, 3],
        )

    def o_copy(slot, head, k):
        peer = lax.rem(place + k, ways)
        return to_z(
            heads_d.at[slot, aligned(peer * rows, rows, rows), aligned(head * HD, HD)],
            land_o.at[slot, :, aligned(place * local + head * HD, HD)],
            o_send.at[slot, head, k - 1], o_recv.at[slot, head, k - 1], k,
        )

    def o_own(slot):
        return pltpu.make_async_copy(
            heads_d.at[slot, my_rows, :], land_o.at[slot, :, aligned(place * local, local)],
            own_sem.at[slot, 4],
        )

    def grad_copy(slot, member, k):
        peer = lax.rem(place + k, ways)
        return to_z(
            tok.at[slot, aligned(peer * rows, rows, rows), pl.ds(member * local, local)],
            grad_ref.at[slot, :, aligned(member * width + place * local, local)],
            g_send.at[slot, member, k - 1], g_recv.at[slot, member, k - 1], k,
        )

    def grad_own(slot, member):
        return pltpu.make_async_copy(
            tok.at[slot, my_rows, pl.ds(member * local, local)],
            grad_ref.at[slot, :, aligned(member * width + place * local, local)],
            own_sem.at[slot, 5 + member],
        )

    def dp_copy(source, target, which, k):
        peer = lax.rem(group + k, groups)
        return pltpu.make_async_remote_copy(
            source.at[peer], target.at[group],
            dp_send.at[which, k - 1], dp_recv.at[which, k - 1], {"dp": peer}, MESH,
        )

    def spread_start(source, target, which):
        for k in range(1, groups):
            dp_copy(source, target, which, k).start()
        target[group] = source[group]

    def spread_sent(source, target, which):
        for k in range(1, groups):
            dp_copy(source, target, which, k).wait_send()

    def spread_wait(source, target, which):
        for k in range(1, groups):
            dp_copy(source, target, which, k).wait_recv()

    def split_rows(source, slot, target):
        for index in range(groups):
            piece = source[slot].astype(jnp.float32)[index * part:(index + 1) * part]
            target[index] = piece.astype(jnp.bfloat16)

    def merge_rows(source, target, slot):
        merged = source[...].astype(jnp.float32).reshape(rows, width)
        target[slot] = merged.astype(jnp.bfloat16)

    def scale_rows(slot):
        def step(index, carry):
            columns = aligned(index * WIDE, WIDE)
            values = cot[slot, :, columns].astype(jnp.float32) * gate_ref[slot:slot + 1, columns]
            scaled[slot, :, columns] = values.astype(jnp.bfloat16)
            return carry

        lax.fori_loop(0, model // WIDE, step, 0)

    def back_project(slot):
        def step(index, carry):
            columns = aligned(index * BLOCK, BLOCK, BLOCK)
            flat_d[slot, :, columns] = dot(scaled[slot], w[columns, :], 1, 1).astype(jnp.bfloat16)
            return carry

        lax.fori_loop(0, width // BLOCK, step, 0)

    def attend(slot):
        text_len, video_len = text_ref[2 * group + slot], clip_ref[2 * group + slot]
        scale = HD ** (-0.5)
        places = lax.broadcasted_iota(jnp.int32, bias.shape, 0)
        bias[...] = jnp.where(live_places(places, text_len, video_len), 0.0, NEGATIVE)

        def head_step(head, carry):
            columns = aligned(head * HD, HD)
            k_columns = aligned(local + head * HD, HD)
            v_columns = aligned(2 * local + head * HD, HD)

            def step(block, inner):
                span = aligned(block * BLOCK, BLOCK, BLOCK)
                q_rows, d_rows = tok[slot, span, columns], heads_d[slot, span, columns]
                keys, values = tok[slot, :, k_columns], tok[slot, :, v_columns]
                wide_bias = jnp.concatenate([bias[...]] * (BLOCK // HD), axis=1)
                scores = dot(keys, q_rows, 1, 1) * (scale * LOG2E) + wide_bias
                peak = jnp.max(scores, axis=0, keepdims=True)
                weights = jnp.exp2(scores - peak)
                total = jnp.sum(weights, axis=0, keepdims=True)
                spots = block * BLOCK + lax.broadcasted_iota(jnp.int32, (1, BLOCK), 1)
                share = jnp.where(live_places(spots, text_len, video_len), 1.0 / total, 0.0)
                probs = weights * share
                probs_low = probs.astype(jnp.bfloat16)
                attended = dot(values, probs_low, 0, 0).T.astype(jnp.bfloat16)
                products = d_rows.astype(jnp.float32) * attended.astype(jnp.float32)
                row_dots = jnp.sum(products.T, axis=0, keepdims=True)
                d_probs = dot(values, d_rows, 1, 1)
                d_scores = (probs * (d_probs - row_dots)).astype(jnp.bfloat16)
                v_part = dot(probs_low, d_rows, 1, 0)
                k_part = dot(d_scores, q_rows, 1, 0)
                q_part = dot(keys, d_scores, 0, 0).T
                tok[slot, span, columns] = (q_part * scale).astype(jnp.bfloat16)
                heads_d[slot, span, columns] = attended

                @pl.when(block == 0)
                def _():
                    dk_sum[...] = k_part
                    dv_sum[...] = v_part

                @pl.when(block > 0)
                def _():
                    dk_sum[...] += k_part
                    dv_sum[...] += v_part

                return inner

            lax.fori_loop(0, seq_len // BLOCK, step, 0)
            tok[slot, :, k_columns] = (dk_sum[...] * scale).astype(jnp.bfloat16)
            tok[slot, :, v_columns] = dv_sum[...].astype(jnp.bfloat16)
            for k in z_order:
                o_copy(slot, head, k).start()
            return carry

        lax.fori_loop(0, heads, head_step, 0)
        o_own(slot).start()

    def o_wait(slot):
        o_own(slot).wait()
        for head in range(heads):
            for k in z_order:
                o_copy(slot, head, k).wait_recv()

    def qkv_start(slot):
        for member in range(3):
            for k in z_order:
                start(qkv_copy(slot, member, k))
            qkv_own(slot, member).start()

    def d_start(slot):
        for k in z_order:
            d_copy(slot, k).start()
        d_own(slot).start()

    def in_wait(slot):
        for member in range(3):
            qkv_own(slot, member).wait()
            for k in z_order:
                qkv_copy(slot, member, k).wait_recv()
        d_own(slot).wait()
        for k in z_order:
            d_copy(slot, k).wait_recv()

    def grad_start(slot, member):
        for k in z_order:
            start(grad_copy(slot, member, k))
        grad_own(slot, member).start()

    cot_load = pltpu.make_async_copy(cot_ref, cot, load_sem.at[0])
    w_load = pltpu.make_async_copy(w_hbm, w, load_sem.at[1])
    qkv_start(1)
    cot_load.start()
    w_load.start()
    cot_load.wait()
    scale_rows(1)
    w_load.wait()
    back_project(1)
    split_rows(flat_d, 1, parts)
    spread_start(parts, spread, 0)
    scale_rows(0)
    back_project(0)
    spread_wait(parts, spread, 0)
    spread_sent(parts, spread, 0)
    for index in range(groups):
        parts[index] = spread[plan_ref[index]]
    spread_start(parts, home, 1)
    spread_wait(parts, home, 1)
    merge_rows(home, flat_d, 1)
    d_start(1)
    qkv_start(0)
    d_start(0)

    in_wait(1)
    attend(1)
    in_wait(0)
    attend(0)
    for member in range(3):
        grad_start(1, member)
    grad_start(0, 0)

    o_wait(1)
    spread_sent(parts, home, 1)
    split_rows(land_o, 1, parts)
    spread_start(parts, spread, 2)
    spread_wait(parts, spread, 2)
    spread_sent(parts, spread, 2)
    for index in range(groups):
        origin = 0
        for other in range(groups):
            origin = jnp.where(plan_ref[other] == index, other, origin)
        parts[index] = spread[origin]
    spread_start(parts, home, 3)
    o_wait(0)
    spread_wait(parts, home, 3)
    for k in z_order:
        d_copy(0, k).wait_send()
    merge_rows(home, flat_d, 0)

    block_rows = model // groups
    per_step = max(1, 384 // block_rows)
    piece_rows = block_rows // ways

    def weight_step(index):
        columns = aligned(index * (per_step * block_rows), per_step * block_rows)
        value = dot(scaled[0, :, columns], land_o[0], 0, 0)
        value += dot(scaled[1, :, columns], flat_d[0], 0, 0)
        for inner in range(per_step):
            for way in range(ways):
                first = (inner * ways + way) * piece_rows
                partial[index * per_step + inner, way] = (
                    value[first:first + piece_rows].astype(jnp.bfloat16)
                )

    halves = (pl.ds(0, width // 2), pl.ds(width // 2, width // 2))
    orders = (list(range(dp_bits)), [0] + list(range(dp_bits - 1, 0, -1)))
    stages = []
    count = 0
    for stage in range(dp_bits):
        entries = []
        for half in range(2):
            order = orders[half]
            taken = order[:stage + 1]
            bit = order[stage]
            kept = sum((bit_of(group, other) << other for other in order[:stage]), 0)
            for index in range(groups >> (stage + 1)):
                rest = rest_value(index, taken, dp_bits)
                given = kept + (1 - bit_of(group, bit)) * (1 << bit) + rest
                held = kept + bit_of(group, bit) * (1 << bit) + rest
                entries.append((half, bit, index, given, held, count))
                count += 1
        stages.append(entries)

    def landed(stage, index, columns):
        if stage == 0:
            return near.at[index, :, :, columns]
        if stage == 1:
            return mid.at[index, :, :, columns]
        first = sum(groups >> (other + 1) for other in range(2, stage))
        return low.at[first + index, :, :, columns]

    def rs_copy(stage, entry):
        half, bit, index, given, _, number = entry
        partner = group + (1 - 2 * bit_of(group, bit)) * (1 << bit)
        return pltpu.make_async_remote_copy(
            partial.at[given, :, :, halves[half]], landed(stage, index, halves[half]),
            rs_send.at[number], rs_recv.at[number], {"dp": partner}, MESH,
        )

    def rs_start(stage):
        for entry in stages[stage]:
            start(rs_copy(stage, entry))

    def rs_finish(stage):
        for entry in stages[stage]:
            rs_copy(stage, entry).wait_recv()
            half, _, index, _, held, _ = entry
            arrived = landed(stage, index, halves[half])

            def step(way, carry):
                value = partial[held, way, :, halves[half]].astype(jnp.float32)
                value += arrived[way].astype(jnp.float32)
                partial[held, way, :, halves[half]] = value.astype(jnp.bfloat16)
                return carry

            lax.fori_loop(0, ways, step, 0)

    steps = groups // per_step
    mine = bit_of(group, 0)
    if per_step == 1:
        def far_step(index, carry):
            weight_step(2 * index + (1 - mine))
            return carry

        def near_step(index, carry):
            weight_step(2 * index + mine)
            return carry

        lax.fori_loop(0, steps // 2, far_step, 0)
        rs_start(0)
        lax.fori_loop(0, steps // 2, near_step, 0)
    else:
        def any_step(index, carry):
            weight_step(index)
            return carry

        lax.fori_loop(0, steps, any_step, 0)
        rs_start(0)

    def project(slot, rows_ref, row_slot):
        def step(index, carry):
            columns = aligned(index * WIDE, WIDE)
            outputs = dot(rows_ref[row_slot], w[:, columns], 1, 0)
            arriving = cot[slot, :, columns].astype(jnp.float32)
            gate_all[0, slot:slot + 1, columns] = jnp.sum(
                arriving * outputs, axis=0, keepdims=True
            )
            gated = outputs * gate_ref[slot:slot + 1, columns]
            cot[slot, :, columns] = gated.astype(jnp.bfloat16)
            return carry

        lax.fori_loop(0, model // WIDE, step, 0)

    def gate_copy(step, peer):
        return pltpu.make_async_remote_copy(
            gate_all.at[2 * step], gate_all.at[2 * step + 1],
            gate_send.at[step], gate_recv.at[step], {"seq": peer}, MESH,
        )

    rs_finish(0)
    rs_start(1)
    project(0, land_o, 0)
    project(1, flat_d, 0)
    rs_finish(1)
    for stage in range(2, dp_bits):
        rs_start(stage)
        rs_finish(stage)

    z_low = bit_of(place, 0)
    z_high = bit_of(place, 1)
    half_ways = ways // 2

    def near_copy(index):
        return pltpu.make_async_remote_copy(
            partial.at[group, 2 * index + (1 - z_low)], z_near.at[index],
            zw_send.at[index], zw_recv.at[index], {"seq": place + 1 - 2 * z_low}, MESH,
        )

    for index in range(half_ways):
        start(near_copy(index))
    grad_start(0, 1)
    gate_near = gate_copy(0, place + 1 - 2 * z_low)
    start(gate_near)
    for index in range(half_ways):
        near_copy(index).wait_recv()
        held = 2 * index + z_low
        value = partial[group, held].astype(jnp.float32) + z_near[index].astype(jnp.float32)
        partial[group, held] = value.astype(jnp.bfloat16)
    far_copy = pltpu.make_async_remote_copy(
        partial.at[group, 2 * (1 - z_high) + z_low], z_far,
        zw_send.at[half_ways], zw_recv.at[half_ways], {"seq": place + 2 - 4 * z_high}, MESH,
    )
    start(far_copy)
    grad_start(0, 2)
    gate_near.wait_recv()
    gate_all[2] = gate_all[0] + gate_all[1]
    gate_far = gate_copy(1, place + 2 - 4 * z_high)
    start(gate_far)
    gate_far.wait_recv()
    gate_out[...] = gate_all[2] + gate_all[3]
    far_copy.wait_recv()
    weight_out[...] = partial[group, place].astype(jnp.float32) + z_far[...].astype(jnp.float32)

    for slot in (0, 1):
        for member in range(3):
            grad_own(slot, member).wait()
            for k in z_order:
                grad_copy(slot, member, k).wait_recv()
        for head in range(heads):
            for k in z_order:
                o_copy(slot, head, k).wait_send()
    spread_sent(parts, home, 3)
    for k in z_order:
        d_copy(1, k).wait_send()
    for copy in sent:
        copy.wait_send()


def settle_kernel(*refs):
    count = (len(refs) - 1) // 2
    sources, targets, sems = refs[:count], refs[count:2 * count], refs[-1]
    copies = [
        pltpu.make_async_copy(source, target, sems.at[index])
        for index, (source, target) in enumerate(zip(sources, targets))
    ]
    for copy in copies:
        copy.start()
    for copy in copies:
        copy.wait()


def settle(arrays):
    return pl.pallas_call(
        settle_kernel,
        in_specs=[pl.BlockSpec(memory_space=pltpu.VMEM)] * len(arrays),
        out_specs=[pl.BlockSpec(memory_space=pl.ANY)] * len(arrays),
        out_shape=[jax.ShapeDtypeStruct(array.shape, array.dtype) for array in arrays],
        scratch_shapes=[pltpu.SemaphoreType.DMA((len(arrays),))],
        compiler_params=pltpu.CompilerParams(vmem_limit_bytes=2_000_000),
        name="settle",
    )(*arrays)


def body(qkv, gate, cotangent, out_weight, clip_lengths, text_lengths, plan):
    groups, ways = lax.axis_size("dp"), lax.axis_size("seq")
    slots, rows, full = qkv.shape
    width, model = out_weight.shape
    local, heads = width // ways, width // ways // HD
    seq_len, part = rows * ways, rows // groups
    piece = model // groups // ways
    low = jnp.bfloat16
    dp_bits = groups.bit_length() - 1
    reduced = sum(2 * (groups >> (stage + 1)) for stage in range(dp_bits))
    late = max(1, sum(groups >> (stage + 1) for stage in range(2, dp_bits)))
    dma = pltpu.SemaphoreType.DMA
    split = pltpu.VMEM((groups, part, width), low)
    scratch = [
        pltpu.VMEM((width, model), low),
        pltpu.VMEM((slots, rows, model), low),
        pltpu.VMEM((slots, seq_len, 3 * local), low),
        pltpu.VMEM((slots, seq_len, local), low),
        pltpu.VMEM((slots, rows, width), low),
        pltpu.VMEM((slots, rows, width), low),
    ] + [split] * 3 + [
        pltpu.VMEM((groups, ways, piece, width), low),
        pltpu.VMEM((groups // 2, ways, piece, width), low),
        pltpu.VMEM((groups // 4, ways, piece, width), low),
        pltpu.VMEM((late, ways, piece, width), low),
        pltpu.VMEM((ways // 2, piece, width), low),
        pltpu.VMEM((piece, width), low),
        pltpu.VMEM((4, slots, model), jnp.float32),
        pltpu.VMEM((seq_len, HD), jnp.float32),
        pltpu.VMEM((seq_len, HD), jnp.float32),
        pltpu.VMEM((seq_len, HD), jnp.float32),
        dma((2,)), dma((slots, 8)),
    ]
    for shape in (
        (slots, 3, ways - 1), (slots, ways - 1), (slots, heads, ways - 1), (slots, 3, ways - 1),
        (4, groups - 1), (reduced,), (ways // 2 + 1,), (2,),
    ):
        scratch += [dma(shape), dma(shape)]
    smem, vmem, anywhere = (
        pl.BlockSpec(memory_space=space) for space in (pltpu.SMEM, pltpu.VMEM, pl.ANY)
    )
    results = pl.pallas_call(
        functools.partial(block_kernel, groups, ways),
        in_specs=[smem] * 3 + [vmem] + [anywhere] * 3,
        out_specs=[vmem] * 4,
        out_shape=[
            pltpu.VMEM(cotangent.shape, low),
            pltpu.VMEM(gate.shape, jnp.float32),
            pltpu.VMEM((piece, width), jnp.float32),
            pltpu.VMEM(qkv.shape, low),
        ],
        scratch_shapes=scratch,
        compiler_params=pltpu.CompilerParams(
            collective_id=0, has_side_effects=True, vmem_limit_bytes=49_000_000
        ),
        name="attention_half",
    )(clip_lengths, text_lengths, plan, gate, qkv, cotangent, out_weight)
    mixed, gate_grad, weight_rows, qkv_grad = settle(results)
    return mixed, gate_grad, weight_rows.T, qkv_grad


def solution(mesh):
    in_specs = (P("dp", "seq", None), P("dp", None), P("dp", "seq", None), P(), P(), P(), P())
    out_specs = (P("dp", "seq", None), P("dp", None), P(None, ("dp", "seq")), P("dp", "seq", None))
    return jax.shard_map(body, mesh=mesh, in_specs=in_specs, out_specs=out_specs, check_vma=False)
```

```python
import functools
import math

import jax
import jax.numpy as jnp
from jax import lax
from jax.experimental import pallas as pl
from jax.experimental.pallas import tpu as pltpu
from jax.sharding import PartitionSpec as P

HD = 128
TXT = 256
BLOCK = 256
WIDE = 512
NEGATIVE = -1e30
LOG2E = math.log2(math.e)
MESH = pl.DeviceIdType.MESH


def dot(left, right, left_dim, right_dim):
    return lax.dot_general(
        left, right, (((left_dim,), (right_dim,)), ((), ())), preferred_element_type=jnp.float32
    )


def live_places(places, text_len, video_len):
    return (places < text_len) | ((places >= TXT) & (places < TXT + video_len))


def aligned(start, size, unit=128):
    return pl.ds(pl.multiple_of(start, unit), size)


def bit_of(index, bit):
    return (index // (1 << bit)) % 2


def rest_value(count, taken, bits):
    value = 0
    for bit in range(bits):
        if bit not in taken:
            value += (count % 2) << bit
            count //= 2
    return value


def block_kernel(
    groups, ways,
    clip_hbm, text_hbm, plan_hbm, gate_hbm, qkv_ref, cot_ref, w_hbm,
    cot, gate_out, weight_out, grad_ref,
    clip_ref, text_ref, plan_ref, w, gate_ref, scaled, tok, heads_d, flat_d, land_o,
    parts, spread, home,
    partial, near, mid, low, z_near, z_far, gate_all, bias, dk_sum, dv_sum,
    load_sem, own_sem,
    in_send, in_recv, d_send, d_recv, o_send, o_recv, g_send, g_recv,
    dp_send, dp_recv, rs_send, rs_recv, zw_send, zw_recv, gate_send, gate_recv,
):
    group, place = lax.axis_index("dp"), lax.axis_index("seq")
    rows, model = cot.shape[1], cot.shape[2]
    width = flat_d.shape[2]
    local = width // ways
    heads = local // HD
    seq_len = rows * ways
    part = rows // groups
    dp_bits = groups.bit_length() - 1
    z_order = sorted(range(1, ways), key=lambda k: -min(k, ways - k))
    my_rows = aligned(place * rows, rows, rows)

    barrier = pltpu.get_barrier_semaphore()
    for k in range(1, ways):
        pl.semaphore_signal(
            barrier, inc=1, device_id={"seq": lax.rem(place + k, ways)}, device_id_type=MESH
        )
    for k in range(1, groups):
        pl.semaphore_signal(
            barrier, inc=1, device_id={"dp": lax.rem(group + k, groups)}, device_id_type=MESH
        )
    pl.semaphore_wait(barrier, ways + groups - 2)

    sent = []

    def start(copy):
        copy.start()
        sent.append(copy)

    def to_z(source, target, send, recv, k):
        return pltpu.make_async_remote_copy(
            source, target, send, recv, {"seq": lax.rem(place + k, ways)}, MESH
        )

    def qkv_copy(slot, member, k):
        peer = lax.rem(place + k, ways)
        return to_z(
            qkv_ref.at[slot, :, aligned(member * width + peer * local, local)],
            tok.at[slot, my_rows, pl.ds(member * local, local)],
            in_send.at[slot, member, k - 1], in_recv.at[slot, member, k - 1], k,
        )

    def qkv_own(slot, member):
        return pltpu.make_async_copy(
            qkv_ref.at[slot, :, aligned(member * width + place * local, local)],
            tok.at[slot, my_rows, pl.ds(member * local, local)],
            own_sem.at[slot, member],
        )

    def d_copy(slot, k):
        peer = lax.rem(place + k, ways)
        return to_z(
            flat_d.at[slot, :, aligned(peer * local, local)], heads_d.at[slot, my_rows, :],
            d_send.at[slot, k - 1], d_recv.at[slot, k - 1], k,
        )

    def d_own(slot):
        return pltpu.make_async_copy(
            flat_d.at[slot, :, aligned(place * local, local)], heads_d.at[slot, my_rows, :],
            own_sem.at[slot, 3],
        )

    def o_copy(slot, head, k):
        peer = lax.rem(place + k, ways)
        return to_z(
            heads_d.at[slot, aligned(peer * rows, rows, rows), aligned(head * HD, HD)],
            land_o.at[slot, :, aligned(place * local + head * HD, HD)],
            o_send.at[slot, head, k - 1], o_recv.at[slot, head, k - 1], k,
        )

    def o_own(slot):
        return pltpu.make_async_copy(
            heads_d.at[slot, my_rows, :], land_o.at[slot, :, aligned(place * local, local)],
            own_sem.at[slot, 4],
        )

    def grad_copy(slot, member, k):
        peer = lax.rem(place + k, ways)
        return to_z(
            tok.at[slot, aligned(peer * rows, rows, rows), pl.ds(member * local, local)],
            grad_ref.at[slot, :, aligned(member * width + place * local, local)],
            g_send.at[slot, member, k - 1], g_recv.at[slot, member, k - 1], k,
        )

    def grad_own(slot, member):
        return pltpu.make_async_copy(
            tok.at[slot, my_rows, pl.ds(member * local, local)],
            grad_ref.at[slot, :, aligned(member * width + place * local, local)],
            own_sem.at[slot, 5 + member],
        )

    def dp_copy(source, target, which, k):
        peer = lax.rem(group + k, groups)
        return pltpu.make_async_remote_copy(
            source.at[peer], target.at[group],
            dp_send.at[which, k - 1], dp_recv.at[which, k - 1], {"dp": peer}, MESH,
        )

    def spread_start(source, target, which):
        for k in range(1, groups):
            dp_copy(source, target, which, k).start()
        target[group] = source[group]

    def spread_sent(source, target, which):
        for k in range(1, groups):
            dp_copy(source, target, which, k).wait_send()

    def spread_wait(source, target, which):
        for k in range(1, groups):
            dp_copy(source, target, which, k).wait_recv()

    def split_rows(source, slot, target):
        for index in range(groups):
            piece = source[slot].astype(jnp.float32)[index * part:(index + 1) * part]
            target[index] = piece.astype(jnp.bfloat16)

    def merge_rows(source, target, slot):
        merged = source[...].astype(jnp.float32).reshape(rows, width)
        target[slot] = merged.astype(jnp.bfloat16)

    def scale_rows(slot):
        def step(index, carry):
            columns = aligned(index * WIDE, WIDE)
            values = cot[slot, :, columns].astype(jnp.float32) * gate_ref[slot:slot + 1, columns]
            scaled[slot, :, columns] = values.astype(jnp.bfloat16)
            return carry

        lax.fori_loop(0, model // WIDE, step, 0)

    def back_project(slot):
        def step(index, carry):
            columns = aligned(index * BLOCK, BLOCK, BLOCK)
            flat_d[slot, :, columns] = dot(scaled[slot], w[columns, :], 1, 1).astype(jnp.bfloat16)
            return carry

        lax.fori_loop(0, width // BLOCK, step, 0)

    def attend(slot):
        text_len, video_len = text_ref[2 * group + slot], clip_ref[2 * group + slot]
        scale = HD ** (-0.5)
        places = lax.broadcasted_iota(jnp.int32, bias.shape, 0)
        bias[...] = jnp.where(live_places(places, text_len, video_len), 0.0, NEGATIVE)

        def head_step(head, carry):
            columns = aligned(head * HD, HD)
            k_columns = aligned(local + head * HD, HD)
            v_columns = aligned(2 * local + head * HD, HD)

            def step(block, inner):
                span = aligned(block * BLOCK, BLOCK, BLOCK)
                q_rows, d_rows = tok[slot, span, columns], heads_d[slot, span, columns]
                keys, values = tok[slot, :, k_columns], tok[slot, :, v_columns]
                wide_bias = jnp.concatenate([bias[...]] * (BLOCK // HD), axis=1)
                scores = dot(keys, q_rows, 1, 1) * (scale * LOG2E) + wide_bias
                peak = jnp.max(scores, axis=0, keepdims=True)
                weights = jnp.exp2(scores - peak)
                total = jnp.sum(weights, axis=0, keepdims=True)
                spots = block * BLOCK + lax.broadcasted_iota(jnp.int32, (1, BLOCK), 1)
                share = jnp.where(live_places(spots, text_len, video_len), 1.0 / total, 0.0)
                probs = weights * share
                probs_low = probs.astype(jnp.bfloat16)
                attended = dot(values, probs_low, 0, 0).T.astype(jnp.bfloat16)
                products = d_rows.astype(jnp.float32) * attended.astype(jnp.float32)
                row_dots = jnp.sum(products.T, axis=0, keepdims=True)
                d_probs = dot(values, d_rows, 1, 1)
                d_scores = (probs * (d_probs - row_dots)).astype(jnp.bfloat16)
                v_part = dot(probs_low, d_rows, 1, 0)
                k_part = dot(d_scores, q_rows, 1, 0)
                q_part = dot(keys, d_scores, 0, 0).T
                tok[slot, span, columns] = (q_part * scale).astype(jnp.bfloat16)
                heads_d[slot, span, columns] = attended

                @pl.when(block == 0)
                def _():
                    dk_sum[...] = k_part
                    dv_sum[...] = v_part

                @pl.when(block > 0)
                def _():
                    dk_sum[...] += k_part
                    dv_sum[...] += v_part

                return inner

            lax.fori_loop(0, seq_len // BLOCK, step, 0)
            tok[slot, :, k_columns] = (dk_sum[...] * scale).astype(jnp.bfloat16)
            tok[slot, :, v_columns] = dv_sum[...].astype(jnp.bfloat16)
            for k in z_order:
                o_copy(slot, head, k).start()
            return carry

        lax.fori_loop(0, heads, head_step, 0)
        o_own(slot).start()

    def o_wait(slot):
        o_own(slot).wait()
        for head in range(heads):
            for k in z_order:
                o_copy(slot, head, k).wait_recv()

    def qkv_start(slot):
        for member in range(3):
            for k in z_order:
                start(qkv_copy(slot, member, k))
            qkv_own(slot, member).start()

    def d_start(slot):
        for k in z_order:
            d_copy(slot, k).start()
        d_own(slot).start()

    def in_wait(slot):
        for member in range(3):
            qkv_own(slot, member).wait()
            for k in z_order:
                qkv_copy(slot, member, k).wait_recv()
        d_own(slot).wait()
        for k in z_order:
            d_copy(slot, k).wait_recv()

    def grad_start(slot, member):
        for k in z_order:
            start(grad_copy(slot, member, k))
        grad_own(slot, member).start()

    cot_load = pltpu.make_async_copy(cot_ref, cot, load_sem.at[0])
    w_load = pltpu.make_async_copy(w_hbm, w, load_sem.at[1])
    gate_load = pltpu.make_async_copy(gate_hbm, gate_ref, load_sem.at[2])
    qkv_start(1)
    tables = [
        pltpu.make_async_copy(source, target, load_sem.at[3 + index])
        for index, (source, target) in enumerate(
            ((clip_hbm, clip_ref), (text_hbm, text_ref), (plan_hbm, plan_ref))
        )
    ]
    for copy in tables:
        copy.start()
    gate_load.start()
    cot_load.start()
    w_load.start()
    gate_load.wait()
    for copy in tables:
        copy.wait()
    cot_load.wait()
    scale_rows(1)
    w_load.wait()
    back_project(1)
    split_rows(flat_d, 1, parts)
    spread_start(parts, spread, 0)
    scale_rows(0)
    back_project(0)
    spread_wait(parts, spread, 0)
    spread_sent(parts, spread, 0)
    for index in range(groups):
        parts[index] = spread[plan_ref[index]]
    spread_start(parts, home, 1)
    spread_wait(parts, home, 1)
    merge_rows(home, flat_d, 1)
    d_start(1)
    qkv_start(0)
    d_start(0)

    in_wait(1)
    attend(1)
    in_wait(0)
    attend(0)
    for member in range(3):
        grad_start(1, member)
    grad_start(0, 0)

    o_wait(1)
    spread_sent(parts, home, 1)
    split_rows(land_o, 1, parts)
    spread_start(parts, spread, 2)
    spread_wait(parts, spread, 2)
    spread_sent(parts, spread, 2)
    for index in range(groups):
        origin = 0
        for other in range(groups):
            origin = jnp.where(plan_ref[other] == index, other, origin)
        parts[index] = spread[origin]
    spread_start(parts, home, 3)
    o_wait(0)
    spread_wait(parts, home, 3)
    for k in z_order:
        d_copy(0, k).wait_send()
    merge_rows(home, flat_d, 0)

    block_rows = model // groups
    per_step = max(1, 384 // block_rows)
    piece_rows = block_rows // ways

    def weight_step(index):
        columns = aligned(index * (per_step * block_rows), per_step * block_rows)
        value = dot(scaled[0, :, columns], land_o[0], 0, 0)
        value += dot(scaled[1, :, columns], flat_d[0], 0, 0)
        for inner in range(per_step):
            for way in range(ways):
                first = (inner * ways + way) * piece_rows
                partial[index * per_step + inner, way] = (
                    value[first:first + piece_rows].astype(jnp.bfloat16)
                )

    halves = (pl.ds(0, width // 2), pl.ds(width // 2, width // 2))
    orders = (list(range(dp_bits)), [0] + list(range(dp_bits - 1, 0, -1)))
    stages = []
    count = 0
    for stage in range(dp_bits):
        entries = []
        for half in range(2):
            order = orders[half]
            taken = order[:stage + 1]
            bit = order[stage]
            kept = sum((bit_of(group, other) << other for other in order[:stage]), 0)
            for index in range(groups >> (stage + 1)):
                rest = rest_value(index, taken, dp_bits)
                given = kept + (1 - bit_of(group, bit)) * (1 << bit) + rest
                held = kept + bit_of(group, bit) * (1 << bit) + rest
                entries.append((half, bit, index, given, held, count))
                count += 1
        stages.append(entries)

    def landed(stage, index, columns):
        if stage == 0:
            return near.at[index, :, :, columns]
        if stage == 1:
            return mid.at[index, :, :, columns]
        first = sum(groups >> (other + 1) for other in range(2, stage))
        return low.at[first + index, :, :, columns]

    def rs_copy(stage, entry):
        half, bit, index, given, _, number = entry
        partner = group + (1 - 2 * bit_of(group, bit)) * (1 << bit)
        return pltpu.make_async_remote_copy(
            partial.at[given, :, :, halves[half]], landed(stage, index, halves[half]),
            rs_send.at[number], rs_recv.at[number], {"dp": partner}, MESH,
        )

    def rs_start(stage):
        for entry in stages[stage]:
            start(rs_copy(stage, entry))

    def rs_finish(stage):
        for entry in stages[stage]:
            rs_copy(stage, entry).wait_recv()
            half, _, index, _, held, _ = entry
            arrived = landed(stage, index, halves[half])

            def step(way, carry):
                value = partial[held, way, :, halves[half]].astype(jnp.float32)
                value += arrived[way].astype(jnp.float32)
                partial[held, way, :, halves[half]] = value.astype(jnp.bfloat16)
                return carry

            lax.fori_loop(0, ways, step, 0)

    steps = groups // per_step
    mine = bit_of(group, 0)
    if per_step == 1:
        def far_step(index, carry):
            weight_step(2 * index + (1 - mine))
            return carry

        def near_step(index, carry):
            weight_step(2 * index + mine)
            return carry

        lax.fori_loop(0, steps // 2, far_step, 0)
        rs_start(0)
        lax.fori_loop(0, steps // 2, near_step, 0)
    else:
        def any_step(index, carry):
            weight_step(index)
            return carry

        lax.fori_loop(0, steps, any_step, 0)
        rs_start(0)

    def project(slot, rows_ref, row_slot):
        def step(index, carry):
            columns = aligned(index * WIDE, WIDE)
            outputs = dot(rows_ref[row_slot], w[:, columns], 1, 0)
            arriving = cot[slot, :, columns].astype(jnp.float32)
            gate_all[0, slot:slot + 1, columns] = jnp.sum(
                arriving * outputs, axis=0, keepdims=True
            )
            gated = outputs * gate_ref[slot:slot + 1, columns]
            cot[slot, :, columns] = gated.astype(jnp.bfloat16)
            return carry

        lax.fori_loop(0, model // WIDE, step, 0)

    def gate_copy(step, peer):
        return pltpu.make_async_remote_copy(
            gate_all.at[2 * step], gate_all.at[2 * step + 1],
            gate_send.at[step], gate_recv.at[step], {"seq": peer}, MESH,
        )

    rs_finish(0)
    rs_start(1)
    project(0, land_o, 0)
    project(1, flat_d, 0)
    rs_finish(1)
    for stage in range(2, dp_bits):
        rs_start(stage)
        rs_finish(stage)

    z_low = bit_of(place, 0)
    z_high = bit_of(place, 1)
    half_ways = ways // 2

    def near_copy(index):
        return pltpu.make_async_remote_copy(
            partial.at[group, 2 * index + (1 - z_low)], z_near.at[index],
            zw_send.at[index], zw_recv.at[index], {"seq": place + 1 - 2 * z_low}, MESH,
        )

    for index in range(half_ways):
        start(near_copy(index))
    grad_start(0, 1)
    gate_near = gate_copy(0, place + 1 - 2 * z_low)
    start(gate_near)
    for index in range(half_ways):
        near_copy(index).wait_recv()
        held = 2 * index + z_low
        value = partial[group, held].astype(jnp.float32) + z_near[index].astype(jnp.float32)
        partial[group, held] = value.astype(jnp.bfloat16)
    far_copy = pltpu.make_async_remote_copy(
        partial.at[group, 2 * (1 - z_high) + z_low], z_far,
        zw_send.at[half_ways], zw_recv.at[half_ways], {"seq": place + 2 - 4 * z_high}, MESH,
    )
    start(far_copy)
    grad_start(0, 2)
    gate_near.wait_recv()
    gate_all[2] = gate_all[0] + gate_all[1]
    gate_far = gate_copy(1, place + 2 - 4 * z_high)
    start(gate_far)
    gate_far.wait_recv()
    gate_out[...] = gate_all[2] + gate_all[3]
    far_copy.wait_recv()
    weight_out[...] = partial[group, place].astype(jnp.float32) + z_far[...].astype(jnp.float32)

    for slot in (0, 1):
        for member in range(3):
            grad_own(slot, member).wait()
            for k in z_order:
                grad_copy(slot, member, k).wait_recv()
        for head in range(heads):
            for k in z_order:
                o_copy(slot, head, k).wait_send()
    spread_sent(parts, home, 3)
    for k in z_order:
        d_copy(1, k).wait_send()
    for copy in sent:
        copy.wait_send()


def settle_kernel(*refs):
    count = (len(refs) - 1) // 2
    sources, targets, sems = refs[:count], refs[count:2 * count], refs[-1]
    copies = [
        pltpu.make_async_copy(source, target, sems.at[index])
        for index, (source, target) in enumerate(zip(sources, targets))
    ]
    for copy in copies:
        copy.start()
    for copy in copies:
        copy.wait()


def settle(arrays):
    return pl.pallas_call(
        settle_kernel,
        in_specs=[pl.BlockSpec(memory_space=pltpu.VMEM)] * len(arrays),
        out_specs=[pl.BlockSpec(memory_space=pl.ANY)] * len(arrays),
        out_shape=[jax.ShapeDtypeStruct(array.shape, array.dtype) for array in arrays],
        scratch_shapes=[pltpu.SemaphoreType.DMA((len(arrays),))],
        compiler_params=pltpu.CompilerParams(vmem_limit_bytes=2_000_000),
        name="settle",
    )(*arrays)


def body(qkv, gate, cotangent, out_weight, clip_lengths, text_lengths, plan):
    groups, ways = lax.axis_size("dp"), lax.axis_size("seq")
    slots, rows, full = qkv.shape
    width, model = out_weight.shape
    local, heads = width // ways, width // ways // HD
    seq_len, part = rows * ways, rows // groups
    piece = model // groups // ways
    low = jnp.bfloat16
    dp_bits = groups.bit_length() - 1
    reduced = sum(2 * (groups >> (stage + 1)) for stage in range(dp_bits))
    late = max(1, sum(groups >> (stage + 1) for stage in range(2, dp_bits)))
    dma = pltpu.SemaphoreType.DMA
    split = pltpu.VMEM((groups, part, width), low)
    scratch = [
        pltpu.SMEM(clip_lengths.shape, jnp.int32),
        pltpu.SMEM(text_lengths.shape, jnp.int32),
        pltpu.SMEM(plan.shape, jnp.int32),
        pltpu.VMEM((width, model), low),
        pltpu.VMEM((slots, model), jnp.float32),
        pltpu.VMEM((slots, rows, model), low),
        pltpu.VMEM((slots, seq_len, 3 * local), low),
        pltpu.VMEM((slots, seq_len, local), low),
        pltpu.VMEM((slots, rows, width), low),
        pltpu.VMEM((slots, rows, width), low),
    ] + [split] * 3 + [
        pltpu.VMEM((groups, ways, piece, width), low),
        pltpu.VMEM((groups // 2, ways, piece, width), low),
        pltpu.VMEM((groups // 4, ways, piece, width), low),
        pltpu.VMEM((late, ways, piece, width), low),
        pltpu.VMEM((ways // 2, piece, width), low),
        pltpu.VMEM((piece, width), low),
        pltpu.VMEM((4, slots, model), jnp.float32),
        pltpu.VMEM((seq_len, HD), jnp.float32),
        pltpu.VMEM((seq_len, HD), jnp.float32),
        pltpu.VMEM((seq_len, HD), jnp.float32),
        dma((6,)), dma((slots, 8)),
    ]
    for shape in (
        (slots, 3, ways - 1), (slots, ways - 1), (slots, heads, ways - 1), (slots, 3, ways - 1),
        (4, groups - 1), (reduced,), (ways // 2 + 1,), (2,),
    ):
        scratch += [dma(shape), dma(shape)]
    smem, vmem, anywhere = (
        pl.BlockSpec(memory_space=space) for space in (pltpu.SMEM, pltpu.VMEM, pl.ANY)
    )
    results = pl.pallas_call(
        functools.partial(block_kernel, groups, ways),
        in_specs=[anywhere] * 7,
        out_specs=[vmem] * 4,
        out_shape=[
            pltpu.VMEM(cotangent.shape, low),
            pltpu.VMEM(gate.shape, jnp.float32),
            pltpu.VMEM((piece, width), jnp.float32),
            pltpu.VMEM(qkv.shape, low),
        ],
        scratch_shapes=scratch,
        compiler_params=pltpu.CompilerParams(
            collective_id=0, has_side_effects=True, vmem_limit_bytes=49_000_000
        ),
        name="attention_half",
    )(clip_lengths, text_lengths, plan, gate, qkv, cotangent, out_weight)
    mixed, gate_grad, weight_rows, qkv_grad = settle(results)
    return mixed, gate_grad, weight_rows.T, qkv_grad


def solution(mesh):
    in_specs = (P("dp", "seq", None), P("dp", None), P("dp", "seq", None), P(), P(), P(), P())
    out_specs = (P("dp", "seq", None), P("dp", None), P(None, ("dp", "seq")), P("dp", "seq", None))
    return jax.shard_map(body, mesh=mesh, in_specs=in_specs, out_specs=out_specs, check_vma=False)
```
